32 devices in a mesh: row: 4 (over x, core), col: 8 (over z, y).
Axes of the slice: x: 2, y: 2, z: 4, core: 2. Of those that a mesh axis runs over, the one named last changes fastest.
Arguments:
- pressure_rhs: bfloat16 [384, 256, 384], P('col', 'row'), may hold values from -10 to 10, as said below
- scalar_source: bfloat16 [384, 256, 384], P('col', 'row'), may hold values from -10 to 10, as said below
- forward_y: bfloat16 [256, 256], replicated, may hold values from -0.375 to 0.375
- back_y: bfloat16 [256, 256], replicated, may hold values from -0.375 to 0.375
- wall_rates: float32 [256], replicated, may hold values from 0.05 to 4
Outputs:
- pressure: bfloat16 [384, 256, 384], P('col', 'row')
- scalar: bfloat16 [384, 256, 384], P('col', 'row')
The draws below stay inside these ranges and needn't reach their ends.
Inputs may be any that keep to these rules, and one draw needn't show every extreme that they name: `pressure_rhs`: a real field of order one. `scalar_source`: a real field of order one.
All inputs are finite; a program needn't handle non-finite values.
Results may differ from the reference program's by a relative error of at most 0.012.
Values may be sent and summed in bfloat16 or wider, within the bound.
A program may use at most 64 MiB of HBM per device.

```python
import math
import jax
import jax.numpy as jnp
from jax import lax

NX = 384
NY = 256
NZ = 384
KEEP = 256


def rough_field(key):
    return jax.random.truncated_normal(key, -4.0, 4.0, (NZ, NY, NX), jnp.float32).astype(jnp.bfloat16)


def draw_pressure_rhs(key, part):
    return rough_field(jax.random.fold_in(key, 11))


def draw_scalar_source(key, part):
    return rough_field(jax.random.fold_in(key, 23))


def bell_draw(rng, dims, deviation, bound, kind=jnp.bfloat16):
    entries = jax.random.normal(rng, dims, jnp.float32) * deviation
    return jnp.minimum(jnp.maximum(entries, -bound), bound).astype(kind)


def setup_inputs(seed: int = 0) -> dict:
    splits = jax.random.split(jax.random.key(seed), 6)
    return {
        "pressure_rhs": draw_pressure_rhs(jax.random.fold_in(splits[5], 71), 0),
        "scalar_source": draw_scalar_source(jax.random.fold_in(splits[5], 71), 0),
        "forward_y": bell_draw(splits[2], (NY, NY), NY ** -0.5, 0.375),
        "back_y": bell_draw(splits[3], (NY, NY), NY ** -0.5, 0.375),
        "wall_rates": jnp.clip(jnp.exp(jax.random.uniform(splits[4], (NY,), jnp.float32, math.log(0.05), math.log(4.0))), 0.05, 4.0),
    }


diffusion = 0.5

def x_table(width, groups):
    half = width // 2
    per = half // groups
    column = lax.broadcasted_iota(jnp.int32, (width, width), 1)
    place = lax.broadcasted_iota(jnp.int32, (width, width), 0)
    owner = column // (2 * per)
    part = column // per % 2
    mode = owner * per + column % per
    phase = mode * place % width
    angle = phase.astype(jnp.float32) * (2.0 * math.pi / width)
    factor = math.sqrt(2.0 / width)
    return jnp.where(part == 0, factor * jnp.cos(angle), -factor * jnp.sin(angle)).astype(jnp.bfloat16)

def x_back_table(width, groups):
    half = width // 2
    per = half // groups
    line = lax.broadcasted_iota(jnp.int32, (width, width), 0)
    place = lax.broadcasted_iota(jnp.int32, (width, width), 1)
    owner = line // (2 * per)
    part = line // per % 2
    mode = owner * per + line % per
    phase = mode * place % width
    angle = phase.astype(jnp.float32) * (2.0 * math.pi / width)
    weight = jnp.where(mode == 0, 0.5, 1.0) * math.sqrt(2.0 / width)
    return jnp.where(part == 0, weight * jnp.cos(angle), -weight * jnp.sin(angle)).astype(jnp.bfloat16)

def z_tables(wave, length):
    place = lax.iota(jnp.int32, length)
    phase = wave[:, None] * place[None, :] % length
    angle = phase.astype(jnp.float32) * (2.0 * math.pi / length)
    factor = 1.0 / math.sqrt(length)
    return ((factor * jnp.cos(angle)).astype(jnp.bfloat16), (factor * jnp.sin(angle)).astype(jnp.bfloat16))

def solve_field(field, is_scalar, table_x, back_x, cosz, sinz, forward_y, back_y, wall_rates, wave):
    depth, height, width = field.shape
    half = width // 2
    kept = wave.shape[0]
    spectra = jnp.dot(field.astype(jnp.float32).reshape(depth * height, width), table_x.astype(jnp.float32))
    spectra = spectra.astype(jnp.bfloat16).astype(jnp.float32).reshape(depth, height * width)
    first = jnp.dot(cosz.astype(jnp.float32), spectra).reshape(kept, height, 2, half)
    second = jnp.dot(sinz.astype(jnp.float32), spectra).reshape(kept, height, 2, half)
    modes = jnp.stack((first[:, :, 0] + second[:, :, 1], first[:, :, 1] - second[:, :, 0]), axis=2)
    modes = modes.astype(jnp.bfloat16).astype(jnp.float32)
    coeffs = jnp.einsum('jy,kypm->kjpm', forward_y.astype(jnp.float32), modes)
    kx_sq = (lax.iota(jnp.int32, half).astype(jnp.float32) * (2.0 * math.pi / width)) ** 2
    signed = jnp.where(wave < depth // 2, wave, wave - depth)
    kz_sq = (signed.astype(jnp.float32) * (2.0 * math.pi / depth)) ** 2
    wave_sq = kz_sq[:, None] + kx_sq[None, :]
    total = wave_sq[:, None, :] + wall_rates[None, :, None]
    if is_scalar:
        hat = coeffs / (1.0 + diffusion * total)[:, :, None, :]
    else:
        hat = coeffs / (-total)[:, :, None, :]
    hat = hat.astype(jnp.bfloat16).astype(jnp.float32)
    back = jnp.einsum('yj,kjpm->kypm', back_y.astype(jnp.float32), hat)
    back = back.astype(jnp.bfloat16).astype(jnp.float32).reshape(kept, height * width)
    first = jnp.dot(cosz.astype(jnp.float32).T, back).reshape(depth, height, 2, half)
    second = jnp.dot(sinz.astype(jnp.float32).T, back).reshape(depth, height, 2, half)
    lines = jnp.stack((first[:, :, 0] - second[:, :, 1], first[:, :, 1] + second[:, :, 0]), axis=2)
    lines = lines.astype(jnp.bfloat16).astype(jnp.float32).reshape(depth * height, width)
    result = jnp.dot(lines, back_x.astype(jnp.float32))
    return result.astype(jnp.bfloat16).reshape(depth, height, width)

def reference(pressure_rhs, scalar_source, forward_y, back_y, wall_rates):
    table_x = x_table(NX, 1)
    back_x = x_back_table(NX, 1)
    wave = lax.iota(jnp.int32, KEEP)
    wave = jnp.where(wave < KEEP // 2, wave, wave + (NZ - KEEP)).astype(jnp.int32)
    cosz, sinz = z_tables(wave, NZ)
    pressure = solve_field(pressure_rhs, False, table_x, back_x, cosz, sinz, forward_y, back_y, wall_rates, wave)
    scalar = solve_field(scalar_source, True, table_x, back_x, cosz, sinz, forward_y, back_y, wall_rates, wave)
    return (pressure, scalar)
```

```python
import functools
import math

import jax
import jax.numpy as jnp
import numpy as np
from jax import lax
from jax.experimental import pallas as pl
from jax.experimental.pallas import tpu as pltpu
from jax.sharding import PartitionSpec as P

KEEP = 256
CHUNKS = 3
MESH = pl.DeviceIdType.MESH


diffusion = 0.5


def x_table(width, groups):
    half = width // 2
    per = half // groups
    column = lax.broadcasted_iota(jnp.int32, (width, width), 1)
    place = lax.broadcasted_iota(jnp.int32, (width, width), 0)
    owner = column // (2 * per)
    part = column // per % 2
    mode = owner * per + column % per
    phase = mode * place % width
    angle = phase.astype(jnp.float32) * (2.0 * math.pi / width)
    factor = math.sqrt(2.0 / width)
    return jnp.where(part == 0, factor * jnp.cos(angle), -factor * jnp.sin(angle)).astype(
        jnp.bfloat16
    )


def x_back_table(width, groups):
    half = width // 2
    per = half // groups
    line = lax.broadcasted_iota(jnp.int32, (width, width), 0)
    place = lax.broadcasted_iota(jnp.int32, (width, width), 1)
    owner = line // (2 * per)
    part = line // per % 2
    mode = owner * per + line % per
    phase = mode * place % width
    angle = phase.astype(jnp.float32) * (2.0 * math.pi / width)
    weight = jnp.where(mode == 0, 0.5, 1.0) * math.sqrt(2.0 / width)
    return jnp.where(part == 0, weight * jnp.cos(angle), -weight * jnp.sin(angle)).astype(
        jnp.bfloat16
    )


def z_tables(wave, length):
    place = lax.iota(jnp.int32, length)
    phase = wave[:, None] * place[None, :] % length
    angle = phase.astype(jnp.float32) * (2.0 * math.pi / length)
    factor = 1.0 / math.sqrt(length)
    return (
        (factor * jnp.cos(angle)).astype(jnp.bfloat16),
        (factor * jnp.sin(angle)).astype(jnp.bfloat16),
    )


def shards(pressure_rhs, scalar_source, forward_y, back_y, wall_rates):
    rows = lax.axis_size("row")
    cols = lax.axis_size("col")
    row_at = lax.axis_index("row")
    col_at = lax.axis_index("col")
    depth_local, height_local, width = pressure_rhs.shape
    height = forward_y.shape[0]
    depth = depth_local * cols
    per = width // (2 * cols)
    wave = lax.iota(jnp.int32, KEEP)
    wave = jnp.where(wave < KEEP // 2, wave, wave + (depth - KEEP))
    count = wave.shape[0]
    count_local = count // rows
    cosz, sinz = z_tables(wave, depth)
    table_x = x_table(width, cols)
    back_x = x_back_table(width, cols)
    fields = jnp.stack((pressure_rhs, scalar_source))
    spectra = jnp.dot(fields.reshape(-1, width), table_x, preferred_element_type=jnp.float32)
    spectra = spectra.astype(jnp.bfloat16).reshape(2, depth_local, height_local, width)
    block = lax.all_to_all(spectra, "col", split_axis=3, concat_axis=1, tiled=True)
    items = block.shape[2]
    flat = block.reshape(2, depth, -1)
    first = jnp.einsum("fzq,nz->fqn", flat, cosz, preferred_element_type=jnp.float32)
    second = jnp.einsum("fzq,nz->fqn", flat, sinz, preferred_element_type=jnp.float32)
    first = first.reshape(2, items, 2, per, count)
    second = second.reshape(2, items, 2, per, count)
    real = first[:, :, 0] + second[:, :, 1]
    imag = first[:, :, 1] - second[:, :, 0]
    zmodes = jnp.stack((real, imag), axis=2).astype(jnp.bfloat16)
    lines = lax.all_to_all(zmodes, "row", split_axis=4, concat_axis=1, tiled=True)
    coeffs = jnp.einsum(
        "jy,fyq->fjq", forward_y, lines.reshape(2, height, -1), preferred_element_type=jnp.float32
    )
    coeffs = coeffs.reshape(2, height, 2, per, count_local)
    modes_x = col_at * per + lax.iota(jnp.int32, per)
    modes_z = lax.dynamic_slice_in_dim(wave, row_at * count_local, count_local)
    signed = jnp.where(modes_z < depth // 2, modes_z, modes_z - depth)
    alive = (modes_z < KEEP // 2) | (modes_z >= depth - KEEP // 2)
    kx_sq = (modes_x.astype(jnp.float32) * (2.0 * math.pi / width)) ** 2
    kz_sq = (signed.astype(jnp.float32) * (2.0 * math.pi / depth)) ** 2
    wave_sq = kx_sq[:, None] + kz_sq[None, :]
    total = wave_sq[None, :, :] + wall_rates[:, None, None]
    hat_pressure = coeffs[0] / (-total)[:, None]
    hat_scalar = coeffs[1] / (1.0 + diffusion * total)[:, None]
    hats = jnp.where(alive, jnp.stack((hat_pressure, hat_scalar)), 0.0).astype(jnp.bfloat16)
    solved = jnp.einsum(
        "yj,fjq->fyq", back_y, hats.reshape(2, height, -1), preferred_element_type=jnp.float32
    )
    solved = solved.astype(jnp.bfloat16).reshape(2, height, 2, per, count_local)
    block = lax.all_to_all(solved, "row", split_axis=1, concat_axis=4, tiled=True)
    first = jnp.einsum("fypkn,nz->fzypk", block, cosz, preferred_element_type=jnp.float32)
    second = jnp.einsum("fypkn,nz->fzypk", block, sinz, preferred_element_type=jnp.float32)
    real = first[:, :, :, 0] - second[:, :, :, 1]
    imag = first[:, :, :, 1] + second[:, :, :, 0]
    zlines = jnp.stack((real, imag), axis=3).astype(jnp.bfloat16)
    zlines = zlines.reshape(2, depth, height_local, 2 * per)
    block = lax.all_to_all(zlines, "col", split_axis=1, concat_axis=3, tiled=True)
    result = jnp.dot(block.reshape(-1, width), back_x, preferred_element_type=jnp.float32)
    result = result.astype(jnp.bfloat16).reshape(block.shape)
    return (result[0], result[1])


def flip(at, d):
    moved = at
    for bit in range(d.bit_length()):
        step = 1 << bit
        if d & step:
            moved = moved + (1 - 2 * ((at // step) % 2)) * step
    return moved


def order(n):
    return list(range(n - 1, 0, -1))


def transform_kernel(
    dims, f0, f1, tab, gf, gi, wf, wb, rates, hout,
    tmp, send1, recv1, bsend, brecv, esend, erecv, hsend,
    s1s, s1r, s1l, s2s, s2r, s2l, s3s, s3r, s3l, s4s, s4r, s4l,
):
    cols, rows, chunks, mc, zl, yl, height, depth, width = dims
    nl = KEEP // rows
    per = mc * chunks
    lanes = 2 * yl
    qc = 2 * mc
    col_at = lax.axis_index("col")
    row_at = lax.axis_index("row")

    barrier = pltpu.get_barrier_semaphore()
    for d in range(1, cols):
        pl.semaphore_signal(barrier, inc=1, device_id={"col": flip(col_at, d)}, device_id_type=MESH)
    for d in range(1, rows):
        pl.semaphore_signal(barrier, inc=1, device_id={"row": flip(row_at, d)}, device_id_type=MESH)
    pl.semaphore_wait(barrier, cols + rows - 2)

    def exchange(axis, n, at, src, dst, ss, rs, ls, k):
        own = pltpu.make_async_copy(src(at), dst(at), ls.at[k])
        pairs = []
        for d in order(n):
            peer = flip(at, d)
            pairs.append(
                pltpu.make_async_remote_copy(
                    src_ref=src(peer),
                    dst_ref=dst(at),
                    send_sem=ss.at[k, d],
                    recv_sem=rs.at[k, d],
                    device_id={axis: peer},
                    device_id_type=MESH,
                )
            )
        return own, pairs

    def ex1(k):
        return exchange(
            "col", cols, col_at,
            lambda p: send1.at[k, pl.ds(p * qc, qc)],
            lambda p: recv1.at[k, :, pl.ds(pl.multiple_of(p * zl, 16), zl), :],
            s1s, s1r, s1l, k,
        )

    def ex2(k):
        return exchange(
            "row", rows, row_at,
            lambda p: bsend.at[k, :, :, pl.ds(pl.multiple_of(p * nl, 16), nl), :],
            lambda p: brecv.at[k, p],
            s2s, s2r, s2l, k,
        )

    def ex3(k):
        return exchange(
            "row", rows, row_at,
            lambda p: esend.at[k, p],
            lambda p: erecv.at[k, :, :, pl.ds(pl.multiple_of(p * nl, 16), nl), :],
            s3s, s3r, s3l, k,
        )

    def ex4(k):
        return exchange(
            "col", cols, col_at,
            lambda p: hsend.at[k, :, :, pl.ds(pl.multiple_of(p * zl, 16), zl), :],
            lambda p: hout.at[k, p],
            s4s, s4r, s4l, k,
        )

    def begin(ex):
        own, pairs = ex
        for c in pairs:
            c.start()
        own.start()

    def arrive(ex):
        own, pairs = ex
        own.wait()
        for c in pairs:
            c.wait_recv()

    def leave(ex):
        for c in ex[1]:
            c.wait_send()

    def forward(k, carry):
        def block(zb, carry):
            for zi in range(0, 16, 2):
                z = zb * 16 + zi
                lines = jnp.concatenate((f0[z], f1[z], f0[z + 1], f1[z + 1]), axis=0)
                acc = lax.dot_general(
                    tab[k], lines, (((1,), (1,)), ((), ())), preferred_element_type=jnp.float32
                )
                tmp[:, zi, :] = acc[:, :lanes]
                tmp[:, zi + 1, :] = acc[:, lanes:]
            at = pl.multiple_of(zb * 16, 16)
            send1[k, :, pl.ds(at, 16), :] = tmp[...].astype(jnp.bfloat16)
            return carry

        lax.fori_loop(0, zl // 16, block, 0)
        begin(ex1(k))
        return carry

    lax.fori_loop(0, chunks, forward, 0)

    def zforward(k):
        def pair(i, carry):
            m = 2 * i
            x = jnp.concatenate(
                [
                    jnp.concatenate((recv1[k, m + a], recv1[k, mc + m + a]), axis=0)
                    for a in range(2)
                ],
                axis=1,
            )
            b = jnp.dot(gf[...], x, preferred_element_type=jnp.float32).astype(jnp.bfloat16)
            for a in range(2):
                for p in range(2):
                    bsend[k, m + a, p] = b[p * KEEP:(p + 1) * KEEP, a * lanes:(a + 1) * lanes]
            return carry

        lax.fori_loop(0, mc // 2, pair, 0)

    def solve(k):
        n = row_at * nl + lax.broadcasted_iota(jnp.int32, (nl, 1), 0)
        n = jnp.where(n < KEEP // 2, n, n + (depth - KEEP))
        n = jnp.where(n < depth // 2, n, n - depth)
        kz_sq = (n.astype(jnp.float32) * (2.0 * math.pi / depth)) ** 2

        def one(m, carry):
            mode = jnp.full((1, 1), col_at * per + k * mc + m, jnp.int32)
            kx_sq = (mode.astype(jnp.float32) * (2.0 * math.pi / width)) ** 2
            total = (kx_sq + kz_sq) + rates[...]
            field = lax.broadcasted_iota(jnp.int32, total.shape, 1) // height
            inv = 1.0 / jnp.where(field == 0, -total, 1.0 + diffusion * total)
            line = jnp.concatenate(
                [brecv[k, s, m].reshape(2 * nl, lanes) for s in range(rows)], axis=1
            )
            c = jnp.dot(line, wf[...], preferred_element_type=jnp.float32)
            hat = (c * jnp.concatenate((inv, inv), axis=0)).astype(jnp.bfloat16)
            e = jnp.dot(hat, wb[...], preferred_element_type=jnp.float32).astype(jnp.bfloat16)
            for r in range(rows):
                esend[k, r, m] = e[:, r * lanes:(r + 1) * lanes].reshape(2, nl, lanes)
            return carry

        lax.fori_loop(0, mc, one, 0)

    def zback(k):
        def pair(i, carry):
            m = 2 * i
            x = jnp.concatenate(
                [erecv[k, m + a].reshape(2 * KEEP, lanes) for a in range(2)], axis=1
            )
            h = jnp.dot(gi[...], x, preferred_element_type=jnp.float32).astype(jnp.bfloat16)
            for a in range(2):
                for p in range(2):
                    hsend[k, p, m + a] = h[p * depth:(p + 1) * depth, a * lanes:(a + 1) * lanes]
            return carry

        lax.fori_loop(0, mc // 2, pair, 0)

    def middle(k, carry):
        arrive(ex1(k))
        zforward(k)
        begin(ex2(k))
        arrive(ex2(k))
        solve(k)
        begin(ex3(k))
        arrive(ex3(k))
        zback(k)
        begin(ex4(k))
        return carry

    lax.fori_loop(0, chunks, middle, 0)

    def finish(k, carry):
        leave(ex1(k))
        leave(ex2(k))
        leave(ex3(k))
        leave(ex4(k))
        arrive(ex4(k))
        return carry

    lax.fori_loop(0, chunks, finish, 0)


def back_kernel(yl, h, bx, o0, o1, tmp):
    lines = tmp.shape[0]
    lanes = 2 * yl
    tmp[...] = h[...].reshape(tmp.shape).astype(jnp.float32)
    for zi in range(0, tmp.shape[1], 2):
        x = jnp.concatenate((tmp[:, zi, :], tmp[:, zi + 1, :]), axis=1).astype(jnp.bfloat16)
        out = lax.dot_general(
            x, bx[...], (((0,), (0,)), ((), ())), preferred_element_type=jnp.float32
        ).astype(jnp.bfloat16)
        o0[zi] = out[:yl]
        o1[zi] = out[yl:lanes]
        o0[zi + 1] = out[lanes:lanes + yl]
        o1[zi + 1] = out[lanes + yl:]


def tables(cols, chunks, mc, depth, width):
    per = mc * chunks
    mode = np.arange(width // 2).reshape(cols, chunks, mc)
    mode = np.stack((mode, mode), axis=2).transpose(1, 0, 2, 3).reshape(-1)
    part = np.broadcast_to(np.arange(2)[None, None, :, None], (chunks, cols, 2, mc)).reshape(-1)
    place = np.arange(width)
    angle = (mode[:, None] * place[None, :] % width).astype(np.float32) * np.float32(
        2.0 * math.pi / width
    )
    factor = np.float32(math.sqrt(2.0 / width))
    wave_x = np.where(part[:, None] == 0, factor * np.cos(angle), -factor * np.sin(angle))
    weight = np.where(mode == 0, 0.5, 1.0).astype(np.float32)[:, None]
    tab = wave_x.astype(jnp.bfloat16).reshape(chunks, -1, width)
    back = (wave_x * weight).astype(jnp.bfloat16)
    wave = np.arange(KEEP)
    wave = np.where(wave < KEEP // 2, wave, wave + (depth - KEEP))
    angle = (wave[:, None] * np.arange(depth)[None, :] % depth).astype(np.float32) * np.float32(
        2.0 * math.pi / depth
    )
    factor = np.float32(1.0 / math.sqrt(depth))
    c, s = factor * np.cos(angle), factor * np.sin(angle)
    gf = np.block([[c, s], [-s, c]]).astype(jnp.bfloat16)
    gi = np.block([[c.T, -s.T], [s.T, c.T]]).astype(jnp.bfloat16)
    return tab, back, gf, gi


def fused(pressure_rhs, scalar_source, forward_y, back_y, wall_rates):
    rows = lax.axis_size("row")
    cols = lax.axis_size("col")
    zl, yl, width = pressure_rhs.shape
    height = forward_y.shape[0]
    depth = zl * cols
    per = width // (2 * cols)
    chunks = CHUNKS
    mc = per // chunks
    nl = KEEP // rows
    lanes = 2 * yl
    tab, back, gf, gi = tables(cols, chunks, mc, depth, width)
    eye = jnp.eye(2, dtype=jnp.bfloat16)
    wf = forward_y.T.reshape(rows, 1, yl, 1, height) * eye.reshape(1, 2, 1, 2, 1)
    wf = wf.reshape(rows * lanes, 2 * height)
    wb = back_y.T.reshape(1, height, rows, 1, yl) * eye.reshape(2, 1, 1, 2, 1)
    wb = wb.reshape(2 * height, rows * lanes)
    rates = jnp.concatenate((wall_rates, wall_rates)).reshape(1, 2 * height)
    dims = (cols, rows, chunks, mc, zl, yl, height, depth, width)
    bf = jnp.bfloat16
    dma = pltpu.SemaphoreType.DMA
    sems = []
    for n in (cols, rows, rows, cols):
        sems += [dma((chunks, n)), dma((chunks, n)), dma((chunks,))]
    h = pl.pallas_call(
        functools.partial(transform_kernel, dims),
        out_shape=jax.ShapeDtypeStruct((chunks, cols, 2, mc, zl, lanes), bf),
        in_specs=[pl.BlockSpec(memory_space=pltpu.VMEM)] * 8,
        out_specs=pl.BlockSpec(memory_space=pl.ANY),
        scratch_shapes=[
            pltpu.VMEM((cols * 2 * mc, 16, lanes), jnp.float32),
            pltpu.VMEM((chunks, cols * 2 * mc, zl, lanes), bf),
            pltpu.VMEM((chunks, 2 * mc, depth, lanes), bf),
            pltpu.VMEM((chunks, mc, 2, KEEP, lanes), bf),
            pltpu.VMEM((chunks, rows, mc, 2, nl, lanes), bf),
            pltpu.VMEM((chunks, rows, mc, 2, nl, lanes), bf),
            pltpu.VMEM((chunks, mc, 2, KEEP, lanes), bf),
            pltpu.VMEM((chunks, 2, mc, depth, lanes), bf),
        ] + sems,
        compiler_params=pltpu.CompilerParams(
            collective_id=0, has_side_effects=True, vmem_limit_bytes=56 << 20
        ),
    )(pressure_rhs, scalar_source, tab, gf, gi, wf, wb, rates)
    h = h.reshape(width, zl, lanes)
    return pl.pallas_call(
        functools.partial(back_kernel, yl),
        grid=(zl // 16,),
        out_shape=[jax.ShapeDtypeStruct((zl, yl, width), bf)] * 2,
        in_specs=[
            pl.BlockSpec((width, 16, lanes), lambda i: (0, i, 0)),
            pl.BlockSpec((width, width), lambda i: (0, 0)),
        ],
        out_specs=[pl.BlockSpec((16, yl, width), lambda i: (i, 0, 0))] * 2,
        scratch_shapes=[pltpu.VMEM((width, 16, lanes), jnp.float32)],
        compiler_params=pltpu.CompilerParams(vmem_limit_bytes=40 << 20),
    )(h, back)


def fits(rows, cols, pressure_rhs, forward_y):
    depth, height, width = pressure_rhs.shape
    power = rows & (rows - 1) == 0 and cols & (cols - 1) == 0
    if depth % cols or height % rows or width % (2 * cols * CHUNKS) or KEEP % rows:
        return False
    return (
        power
        and (2 * height // rows) % 128 == 0
        and (depth // cols) % 16 == 0
        and (KEEP // rows) % 16 == 0
        and (width // (2 * cols * CHUNKS)) % 2 == 0
    )


def solution(mesh):
    placed = (P("col", "row", None), P("col", "row", None), P(), P(), P())
    rows, cols = mesh.shape["row"], mesh.shape["col"]

    def run(pressure_rhs, scalar_source, forward_y, back_y, wall_rates):
        body = fused if fits(rows, cols, pressure_rhs, forward_y) else shards
        return jax.shard_map(
            body,
            mesh=mesh,
            in_specs=placed,
            out_specs=(P("col", "row", None), P("col", "row", None)),
            check_vma=False,
        )(pressure_rhs, scalar_source, forward_y, back_y, wall_rates)

    return run
```

```python
import functools
import math

import jax
import jax.numpy as jnp
import numpy as np
from jax import lax
from jax.experimental import pallas as pl
from jax.experimental.pallas import tpu as pltpu
from jax.sharding import PartitionSpec as P

KEEP = 256
CHUNKS = 3
MESH = pl.DeviceIdType.MESH


diffusion = 0.5


def x_table(width, groups):
    half = width // 2
    per = half // groups
    column = lax.broadcasted_iota(jnp.int32, (width, width), 1)
    place = lax.broadcasted_iota(jnp.int32, (width, width), 0)
    owner = column // (2 * per)
    part = column // per % 2
    mode = owner * per + column % per
    phase = mode * place % width
    angle = phase.astype(jnp.float32) * (2.0 * math.pi / width)
    factor = math.sqrt(2.0 / width)
    return jnp.where(part == 0, factor * jnp.cos(angle), -factor * jnp.sin(angle)).astype(
        jnp.bfloat16
    )


def x_back_table(width, groups):
    half = width // 2
    per = half // groups
    line = lax.broadcasted_iota(jnp.int32, (width, width), 0)
    place = lax.broadcasted_iota(jnp.int32, (width, width), 1)
    owner = line // (2 * per)
    part = line // per % 2
    mode = owner * per + line % per
    phase = mode * place % width
    angle = phase.astype(jnp.float32) * (2.0 * math.pi / width)
    weight = jnp.where(mode == 0, 0.5, 1.0) * math.sqrt(2.0 / width)
    return jnp.where(part == 0, weight * jnp.cos(angle), -weight * jnp.sin(angle)).astype(
        jnp.bfloat16
    )


def z_tables(wave, length):
    place = lax.iota(jnp.int32, length)
    phase = wave[:, None] * place[None, :] % length
    angle = phase.astype(jnp.float32) * (2.0 * math.pi / length)
    factor = 1.0 / math.sqrt(length)
    return (
        (factor * jnp.cos(angle)).astype(jnp.bfloat16),
        (factor * jnp.sin(angle)).astype(jnp.bfloat16),
    )


def shards(pressure_rhs, scalar_source, forward_y, back_y, wall_rates):
    rows = lax.axis_size("row")
    cols = lax.axis_size("col")
    row_at = lax.axis_index("row")
    col_at = lax.axis_index("col")
    depth_local, height_local, width = pressure_rhs.shape
    height = forward_y.shape[0]
    depth = depth_local * cols
    per = width // (2 * cols)
    wave = lax.iota(jnp.int32, KEEP)
    wave = jnp.where(wave < KEEP // 2, wave, wave + (depth - KEEP))
    count = wave.shape[0]
    count_local = count // rows
    cosz, sinz = z_tables(wave, depth)
    table_x = x_table(width, cols)
    back_x = x_back_table(width, cols)
    fields = jnp.stack((pressure_rhs, scalar_source))
    spectra = jnp.dot(fields.reshape(-1, width), table_x, preferred_element_type=jnp.float32)
    spectra = spectra.astype(jnp.bfloat16).reshape(2, depth_local, height_local, width)
    block = lax.all_to_all(spectra, "col", split_axis=3, concat_axis=1, tiled=True)
    items = block.shape[2]
    flat = block.reshape(2, depth, -1)
    first = jnp.einsum("fzq,nz->fqn", flat, cosz, preferred_element_type=jnp.float32)
    second = jnp.einsum("fzq,nz->fqn", flat, sinz, preferred_element_type=jnp.float32)
    first = first.reshape(2, items, 2, per, count)
    second = second.reshape(2, items, 2, per, count)
    real = first[:, :, 0] + second[:, :, 1]
    imag = first[:, :, 1] - second[:, :, 0]
    zmodes = jnp.stack((real, imag), axis=2).astype(jnp.bfloat16)
    lines = lax.all_to_all(zmodes, "row", split_axis=4, concat_axis=1, tiled=True)
    coeffs = jnp.einsum(
        "jy,fyq->fjq", forward_y, lines.reshape(2, height, -1), preferred_element_type=jnp.float32
    )
    coeffs = coeffs.reshape(2, height, 2, per, count_local)
    modes_x = col_at * per + lax.iota(jnp.int32, per)
    modes_z = lax.dynamic_slice_in_dim(wave, row_at * count_local, count_local)
    signed = jnp.where(modes_z < depth // 2, modes_z, modes_z - depth)
    alive = (modes_z < KEEP // 2) | (modes_z >= depth - KEEP // 2)
    kx_sq = (modes_x.astype(jnp.float32) * (2.0 * math.pi / width)) ** 2
    kz_sq = (signed.astype(jnp.float32) * (2.0 * math.pi / depth)) ** 2
    wave_sq = kx_sq[:, None] + kz_sq[None, :]
    total = wave_sq[None, :, :] + wall_rates[:, None, None]
    hat_pressure = coeffs[0] / (-total)[:, None]
    hat_scalar = coeffs[1] / (1.0 + diffusion * total)[:, None]
    hats = jnp.where(alive, jnp.stack((hat_pressure, hat_scalar)), 0.0).astype(jnp.bfloat16)
    solved = jnp.einsum(
        "yj,fjq->fyq", back_y, hats.reshape(2, height, -1), preferred_element_type=jnp.float32
    )
    solved = solved.astype(jnp.bfloat16).reshape(2, height, 2, per, count_local)
    block = lax.all_to_all(solved, "row", split_axis=1, concat_axis=4, tiled=True)
    first = jnp.einsum("fypkn,nz->fzypk", block, cosz, preferred_element_type=jnp.float32)
    second = jnp.einsum("fypkn,nz->fzypk", block, sinz, preferred_element_type=jnp.float32)
    real = first[:, :, :, 0] - second[:, :, :, 1]
    imag = first[:, :, :, 1] + second[:, :, :, 0]
    zlines = jnp.stack((real, imag), axis=3).astype(jnp.bfloat16)
    zlines = zlines.reshape(2, depth, height_local, 2 * per)
    block = lax.all_to_all(zlines, "col", split_axis=1, concat_axis=3, tiled=True)
    result = jnp.dot(block.reshape(-1, width), back_x, preferred_element_type=jnp.float32)
    result = result.astype(jnp.bfloat16).reshape(block.shape)
    return (result[0], result[1])


def flip(at, d):
    moved = at
    for bit in range(d.bit_length()):
        step = 1 << bit
        if d & step:
            moved = moved + (1 - 2 * ((at // step) % 2)) * step
    return moved


def order(n):
    return list(range(n - 1, 0, -1))


def transform_kernel(
    dims, p_hbm, s_hbm, tab_hbm, gf_hbm, gi_hbm, bx_hbm, fy, by, rates, po_hbm, so_hbm,
    f0, f1, tab, gf, gi, bx, wf, wb,
    tmp, send1, recv1, bsend, brecv, esend, erecv, hsend, hrecv, acc,
    in_sem, tab_sem, out_sem,
    s1s, s1r, s1l, s2s, s2r, s2l, s3s, s3r, s3l, s4s, s4r, s4l,
):
    cols, rows, chunks, mc, zl, yl, height, depth, width = dims
    nl = KEEP // rows
    per = mc * chunks
    lanes = 2 * yl
    qc = 2 * mc
    blocks = zl // 16
    col_at = lax.axis_index("col")
    row_at = lax.axis_index("row")

    def span(zb):
        return pl.ds(pl.multiple_of(zb * 16, 16), 16)

    def load(field, zb):
        src, dst = ((p_hbm, f0), (s_hbm, f1))[field]
        return pltpu.make_async_copy(src.at[span(zb)], dst.at[span(zb)], in_sem.at[field, zb])

    def store(field, zb):
        src, dst = ((f0, po_hbm), (f1, so_hbm))[field]
        return pltpu.make_async_copy(src.at[span(zb)], dst.at[span(zb)], out_sem.at[field, zb])

    consts = [
        pltpu.make_async_copy(src, dst, tab_sem.at[i])
        for i, (src, dst) in enumerate(((tab_hbm, tab), (gf_hbm, gf), (gi_hbm, gi), (bx_hbm, bx)))
    ]
    consts[0].start()
    for zb in range(blocks):
        load(0, zb).start()
        load(1, zb).start()
    for c in consts[1:]:
        c.start()

    barrier = pltpu.get_barrier_semaphore()
    for d in range(1, cols):
        pl.semaphore_signal(barrier, inc=1, device_id={"col": flip(col_at, d)}, device_id_type=MESH)
    for d in range(1, rows):
        pl.semaphore_signal(barrier, inc=1, device_id={"row": flip(row_at, d)}, device_id_type=MESH)
    pl.semaphore_wait(barrier, cols + rows - 2)

    def exchange(axis, n, at, src, dst, ss, rs, ls, k):
        own = lambda: pltpu.make_async_copy(src(at), dst(at), ls.at[k])
        pairs = []
        for d in order(n):
            peer = flip(at, d)
            pairs.append(
                pltpu.make_async_remote_copy(
                    src_ref=src(peer),
                    dst_ref=dst(at),
                    send_sem=ss.at[k, d],
                    recv_sem=rs.at[k, d],
                    device_id={axis: peer},
                    device_id_type=MESH,
                )
            )
        return own, pairs

    def ex1(k, zb):
        return exchange(
            "col", cols, col_at,
            lambda p: send1.at[k, pl.ds(p * qc, qc), span(zb), :],
            lambda p: recv1.at[k, :, pl.ds(pl.multiple_of(p * zl + zb * 16, 16), 16), :],
            s1s, s1r, s1l, k * blocks + zb,
        )

    def ex2(k):
        return exchange(
            "row", rows, row_at,
            lambda p: bsend.at[k, :, :, pl.ds(pl.multiple_of(p * nl, 16), nl), :],
            lambda p: brecv.at[k, p],
            s2s, s2r, s2l, k,
        )

    def ex3(k):
        return exchange(
            "row", rows, row_at,
            lambda p: esend.at[k, p],
            lambda p: erecv.at[k, :, :, pl.ds(pl.multiple_of(p * nl, 16), nl), :],
            s3s, s3r, s3l, k,
        )

    def ex4(k, zb):
        return exchange(
            "col", cols, col_at,
            lambda p: hsend.at[k, :, :, pl.ds(pl.multiple_of(p * zl + zb * 16, 16), 16), :],
            lambda p: hrecv.at[k, p, :, :, span(zb), :],
            s4s, s4r, s4l, k * blocks + zb,
        )

    def begin(ex):
        own, pairs = ex
        for c in pairs:
            c.start()
        own().start()

    def arrive(ex):
        own, pairs = ex
        own().wait()
        for c in pairs:
            c.wait_recv()

    def leave(ex):
        for c in ex[1]:
            c.wait_send()

    consts[0].wait()

    def forward(i, carry):
        k, zb = i // blocks, i % blocks

        @pl.when(k == 0)
        def _():
            load(0, zb).wait()
            load(1, zb).wait()

        for zi in range(0, 16, 2):
            z = zb * 16 + zi
            lines = jnp.concatenate((f0[z], f1[z], f0[z + 1], f1[z + 1]), axis=0)
            out = lax.dot_general(
                tab[k], lines, (((1,), (1,)), ((), ())), preferred_element_type=jnp.float32
            )
            tmp[:, zi, :] = out[:, :lanes]
            tmp[:, zi + 1, :] = out[:, lanes:]
        send1[k, :, span(zb), :] = tmp[...].astype(jnp.bfloat16)
        begin(ex1(k, zb))
        return carry

    lax.fori_loop(0, chunks * blocks, forward, 0)
    for c in consts[1:]:
        c.wait()

    wf[...] = jnp.zeros_like(wf)
    lines = fy[...].T
    for s in range(rows):
        for f in range(2):
            wf[s * lanes + f * yl:s * lanes + (f + 1) * yl, f * height:(f + 1) * height] = lines[
                s * yl:(s + 1) * yl
            ]
    lines = by[...].T
    blank = jnp.zeros((height, yl), jnp.bfloat16)
    for r in range(rows):
        part = lines[:, r * yl:(r + 1) * yl]
        wb[:height, r * lanes:(r + 1) * lanes] = jnp.concatenate((part, blank), axis=1)
        wb[height:, r * lanes:(r + 1) * lanes] = jnp.concatenate((blank, part), axis=1)

    def zforward(k):
        def pair(i, carry):
            m = 2 * i
            x = jnp.concatenate(
                [
                    jnp.concatenate((recv1[k, m + a], recv1[k, mc + m + a]), axis=0)
                    for a in range(2)
                ],
                axis=1,
            )
            b = jnp.dot(gf[...], x, preferred_element_type=jnp.float32).astype(jnp.bfloat16)
            for a in range(2):
                for p in range(2):
                    bsend[k, m + a, p] = b[p * KEEP:(p + 1) * KEEP, a * lanes:(a + 1) * lanes]
            return carry

        lax.fori_loop(0, mc // 2, pair, 0)

    def solve(k):
        n = row_at * nl + lax.broadcasted_iota(jnp.int32, (nl, 1), 0)
        n = jnp.where(n < KEEP // 2, n, n + (depth - KEEP))
        n = jnp.where(n < depth // 2, n, n - depth)
        kz_sq = (n.astype(jnp.float32) * (2.0 * math.pi / depth)) ** 2

        def one(m, carry):
            mode = jnp.full((1, 1), col_at * per + k * mc + m, jnp.int32)
            kx_sq = (mode.astype(jnp.float32) * (2.0 * math.pi / width)) ** 2
            total = (kx_sq + kz_sq) + jnp.concatenate((rates[...], rates[...]), axis=1)
            field = lax.broadcasted_iota(jnp.int32, total.shape, 1) // height
            inv = 1.0 / jnp.where(field == 0, -total, 1.0 + diffusion * total)
            line = jnp.concatenate(
                [brecv[k, s, m].reshape(2 * nl, lanes) for s in range(rows)], axis=1
            )
            c = jnp.dot(line, wf[...], preferred_element_type=jnp.float32)
            hat = (c * jnp.concatenate((inv, inv), axis=0)).astype(jnp.bfloat16)
            e = jnp.dot(hat, wb[...], preferred_element_type=jnp.float32).astype(jnp.bfloat16)
            for r in range(rows):
                esend[k, r, m] = e[:, r * lanes:(r + 1) * lanes].reshape(2, nl, lanes)
            return carry

        lax.fori_loop(0, mc, one, 0)

    def zback(k):
        def pair(i, carry):
            m = 2 * i
            x = jnp.concatenate(
                [erecv[k, m + a].reshape(2 * KEEP, lanes) for a in range(2)], axis=1
            )
            h = jnp.dot(gi[...], x, preferred_element_type=jnp.float32).astype(jnp.bfloat16)
            for a in range(2):
                for p in range(2):
                    hsend[k, p, m + a] = h[p * depth:(p + 1) * depth, a * lanes:(a + 1) * lanes]
            return carry

        lax.fori_loop(0, mc // 2, pair, 0)

    def each(k, act):
        def one(zb, carry):
            act(k, zb)
            return carry

        lax.fori_loop(0, blocks, one, 0)

    def middle(k, carry):
        each(k, lambda k, zb: arrive(ex1(k, zb)))
        zforward(k)
        begin(ex2(k))
        arrive(ex2(k))
        solve(k)
        begin(ex3(k))
        arrive(ex3(k))
        zback(k)
        each(k, lambda k, zb: begin(ex4(k, zb)))
        return carry

    lax.fori_loop(0, chunks, middle, 0)

    def result(k, zb):
        arrive(ex4(k, zb))
        tmp[...] = hrecv[k, :, :, :, span(zb), :].reshape(tmp.shape).astype(jnp.float32)
        for zi in range(0, 16, 2):
            z = zb * 16 + zi
            x = jnp.concatenate((tmp[:, zi, :], tmp[:, zi + 1, :]), axis=1).astype(jnp.bfloat16)
            out = lax.dot_general(
                x, bx[k], (((0,), (0,)), ((), ())), preferred_element_type=jnp.float32
            )
            for a in range(2):
                half = out[a * lanes:(a + 1) * lanes]
                if k > 0:
                    half = acc[z + a] + half
                if k < chunks - 1:
                    acc[z + a] = half
                else:
                    f0[z + a] = half[:yl].astype(jnp.bfloat16)
                    f1[z + a] = half[yl:].astype(jnp.bfloat16)
        if k == chunks - 1:
            store(0, zb).start()
            store(1, zb).start()

    for k in range(chunks):
        each(k, result)

    def finish(k, carry):
        each(k, lambda k, zb: leave(ex1(k, zb)))
        leave(ex2(k))
        leave(ex3(k))
        each(k, lambda k, zb: leave(ex4(k, zb)))
        return carry

    lax.fori_loop(0, chunks, finish, 0)
    for zb in range(blocks):
        store(0, zb).wait()
        store(1, zb).wait()


def tables(cols, chunks, mc, depth, width):
    per = mc * chunks
    mode = np.arange(width // 2).reshape(cols, chunks, mc)
    mode = np.stack((mode, mode), axis=2).transpose(1, 0, 2, 3).reshape(-1)
    part = np.broadcast_to(np.arange(2)[None, None, :, None], (chunks, cols, 2, mc)).reshape(-1)
    place = np.arange(width)
    angle = (mode[:, None] * place[None, :] % width).astype(np.float32) * np.float32(
        2.0 * math.pi / width
    )
    factor = np.float32(math.sqrt(2.0 / width))
    wave_x = np.where(part[:, None] == 0, factor * np.cos(angle), -factor * np.sin(angle))
    weight = np.where(mode == 0, 0.5, 1.0).astype(np.float32)[:, None]
    tab = wave_x.astype(jnp.bfloat16).reshape(chunks, -1, width)
    back = (wave_x * weight).astype(jnp.bfloat16).reshape(chunks, -1, width)
    wave = np.arange(KEEP)
    wave = np.where(wave < KEEP // 2, wave, wave + (depth - KEEP))
    angle = (wave[:, None] * np.arange(depth)[None, :] % depth).astype(np.float32) * np.float32(
        2.0 * math.pi / depth
    )
    factor = np.float32(1.0 / math.sqrt(depth))
    c, s = factor * np.cos(angle), factor * np.sin(angle)
    gf = np.block([[c, s], [-s, c]]).astype(jnp.bfloat16)
    gi = np.block([[c.T, -s.T], [s.T, c.T]]).astype(jnp.bfloat16)
    return tab, back, gf, gi


def fused(pressure_rhs, scalar_source, forward_y, back_y, wall_rates):
    rows = lax.axis_size("row")
    cols = lax.axis_size("col")
    zl, yl, width = pressure_rhs.shape
    height = forward_y.shape[0]
    depth = zl * cols
    per = width // (2 * cols)
    chunks = CHUNKS
    mc = per // chunks
    nl = KEEP // rows
    lanes = 2 * yl
    tab, back, gf, gi = tables(cols, chunks, mc, depth, width)
    rates = wall_rates.reshape(1, height)
    dims = (cols, rows, chunks, mc, zl, yl, height, depth, width)
    bf = jnp.bfloat16
    dma = pltpu.SemaphoreType.DMA
    blocks = zl // 16
    sems = [dma((2, blocks)), dma((4,)), dma((2, blocks))]
    for n, steps in ((cols, chunks * blocks), (rows, chunks), (rows, chunks), (cols, chunks * blocks)):
        sems += [dma((steps, n)), dma((steps, n)), dma((steps,))]
    field = jax.ShapeDtypeStruct((zl, yl, width), bf)
    anywhere = pl.BlockSpec(memory_space=pl.ANY)
    inside = pl.BlockSpec(memory_space=pltpu.VMEM)
    vmem = [
        (field.shape, bf),
        (field.shape, bf),
        (tab.shape, bf),
        (gf.shape, bf),
        (gi.shape, bf),
        (back.shape, bf),
        ((rows * lanes, 2 * height), bf),
        ((2 * height, rows * lanes), bf),
        ((cols * 2 * mc, 16, lanes), jnp.float32),
        ((chunks, cols * 2 * mc, zl, lanes), bf),
        ((chunks, 2 * mc, depth, lanes), bf),
        ((chunks, mc, 2, KEEP, lanes), bf),
        ((chunks, rows, mc, 2, nl, lanes), bf),
        ((chunks, rows, mc, 2, nl, lanes), bf),
        ((chunks, mc, 2, KEEP, lanes), bf),
        ((chunks, 2, mc, depth, lanes), bf),
        ((chunks, cols, 2, mc, zl, lanes), bf),
        ((zl, lanes, width), jnp.float32),
    ]
    return tuple(
        pl.pallas_call(
            functools.partial(transform_kernel, dims),
            out_shape=[field, field],
            in_specs=[anywhere] * 6 + [inside] * 3,
            out_specs=[anywhere] * 2,
            scratch_shapes=[pltpu.VMEM(*v) for v in vmem] + sems,
            compiler_params=pltpu.CompilerParams(
                collective_id=0, has_side_effects=True, vmem_limit_bytes=67043328
            ),
        )(pressure_rhs, scalar_source, tab, gf, gi, back, forward_y, back_y, rates)
    )


def fits(rows, cols, pressure_rhs, forward_y):
    depth, height, width = pressure_rhs.shape
    power = rows & (rows - 1) == 0 and cols & (cols - 1) == 0
    if depth % cols or height % rows or width % (2 * cols * CHUNKS) or KEEP % rows:
        return False
    return (
        power
        and (2 * height // rows) % 128 == 0
        and (depth // cols) % 16 == 0
        and (KEEP // rows) % 16 == 0
        and (width // (2 * cols * CHUNKS)) % 2 == 0
    )


def solution(mesh):
    placed = (P("col", "row", None), P("col", "row", None), P(), P(), P())
    rows, cols = mesh.shape["row"], mesh.shape["col"]

    def run(pressure_rhs, scalar_source, forward_y, back_y, wall_rates):
        body = fused if fits(rows, cols, pressure_rhs, forward_y) else shards
        return jax.shard_map(
            body,
            mesh=mesh,
            in_specs=placed,
            out_specs=(P("col", "row", None), P("col", "row", None)),
            check_vma=False,
        )(pressure_rhs, scalar_source, forward_y, back_y, wall_rates)

    return run
```

```python
import functools
import math

import jax
import jax.numpy as jnp
import numpy as np
from jax import lax
from jax.experimental import pallas as pl
from jax.experimental.pallas import tpu as pltpu
from jax.sharding import PartitionSpec as P

KEEP = 256
CHUNKS = 3
MESH = pl.DeviceIdType.MESH


diffusion = 0.5


def x_table(width, groups):
    half = width // 2
    per = half // groups
    column = lax.broadcasted_iota(jnp.int32, (width, width), 1)
    place = lax.broadcasted_iota(jnp.int32, (width, width), 0)
    owner = column // (2 * per)
    part = column // per % 2
    mode = owner * per + column % per
    phase = mode * place % width
    angle = phase.astype(jnp.float32) * (2.0 * math.pi / width)
    factor = math.sqrt(2.0 / width)
    return jnp.where(part == 0, factor * jnp.cos(angle), -factor * jnp.sin(angle)).astype(
        jnp.bfloat16
    )


def x_back_table(width, groups):
    half = width // 2
    per = half // groups
    line = lax.broadcasted_iota(jnp.int32, (width, width), 0)
    place = lax.broadcasted_iota(jnp.int32, (width, width), 1)
    owner = line // (2 * per)
    part = line // per % 2
    mode = owner * per + line % per
    phase = mode * place % width
    angle = phase.astype(jnp.float32) * (2.0 * math.pi / width)
    weight = jnp.where(mode == 0, 0.5, 1.0) * math.sqrt(2.0 / width)
    return jnp.where(part == 0, weight * jnp.cos(angle), -weight * jnp.sin(angle)).astype(
        jnp.bfloat16
    )


def z_tables(wave, length):
    place = lax.iota(jnp.int32, length)
    phase = wave[:, None] * place[None, :] % length
    angle = phase.astype(jnp.float32) * (2.0 * math.pi / length)
    factor = 1.0 / math.sqrt(length)
    return (
        (factor * jnp.cos(angle)).astype(jnp.bfloat16),
        (factor * jnp.sin(angle)).astype(jnp.bfloat16),
    )


def shards(pressure_rhs, scalar_source, forward_y, back_y, wall_rates):
    rows = lax.axis_size("row")
    cols = lax.axis_size("col")
    row_at = lax.axis_index("row")
    col_at = lax.axis_index("col")
    depth_local, height_local, width = pressure_rhs.shape
    height = forward_y.shape[0]
    depth = depth_local * cols
    per = width // (2 * cols)
    wave = lax.iota(jnp.int32, KEEP)
    wave = jnp.where(wave < KEEP // 2, wave, wave + (depth - KEEP))
    count = wave.shape[0]
    count_local = count // rows
    cosz, sinz = z_tables(wave, depth)
    table_x = x_table(width, cols)
    back_x = x_back_table(width, cols)
    fields = jnp.stack((pressure_rhs, scalar_source))
    spectra = jnp.dot(fields.reshape(-1, width), table_x, preferred_element_type=jnp.float32)
    spectra = spectra.astype(jnp.bfloat16).reshape(2, depth_local, height_local, width)
    block = lax.all_to_all(spectra, "col", split_axis=3, concat_axis=1, tiled=True)
    items = block.shape[2]
    flat = block.reshape(2, depth, -1)
    first = jnp.einsum("fzq,nz->fqn", flat, cosz, preferred_element_type=jnp.float32)
    second = jnp.einsum("fzq,nz->fqn", flat, sinz, preferred_element_type=jnp.float32)
    first = first.reshape(2, items, 2, per, count)
    second = second.reshape(2, items, 2, per, count)
    real = first[:, :, 0] + second[:, :, 1]
    imag = first[:, :, 1] - second[:, :, 0]
    zmodes = jnp.stack((real, imag), axis=2).astype(jnp.bfloat16)
    lines = lax.all_to_all(zmodes, "row", split_axis=4, concat_axis=1, tiled=True)
    coeffs = jnp.einsum(
        "jy,fyq->fjq", forward_y, lines.reshape(2, height, -1), preferred_element_type=jnp.float32
    )
    coeffs = coeffs.reshape(2, height, 2, per, count_local)
    modes_x = col_at * per + lax.iota(jnp.int32, per)
    modes_z = lax.dynamic_slice_in_dim(wave, row_at * count_local, count_local)
    signed = jnp.where(modes_z < depth // 2, modes_z, modes_z - depth)
    alive = (modes_z < KEEP // 2) | (modes_z >= depth - KEEP // 2)
    kx_sq = (modes_x.astype(jnp.float32) * (2.0 * math.pi / width)) ** 2
    kz_sq = (signed.astype(jnp.float32) * (2.0 * math.pi / depth)) ** 2
    wave_sq = kx_sq[:, None] + kz_sq[None, :]
    total = wave_sq[None, :, :] + wall_rates[:, None, None]
    hat_pressure = coeffs[0] / (-total)[:, None]
    hat_scalar = coeffs[1] / (1.0 + diffusion * total)[:, None]
    hats = jnp.where(alive, jnp.stack((hat_pressure, hat_scalar)), 0.0).astype(jnp.bfloat16)
    solved = jnp.einsum(
        "yj,fjq->fyq", back_y, hats.reshape(2, height, -1), preferred_element_type=jnp.float32
    )
    solved = solved.astype(jnp.bfloat16).reshape(2, height, 2, per, count_local)
    block = lax.all_to_all(solved, "row", split_axis=1, concat_axis=4, tiled=True)
    first = jnp.einsum("fypkn,nz->fzypk", block, cosz, preferred_element_type=jnp.float32)
    second = jnp.einsum("fypkn,nz->fzypk", block, sinz, preferred_element_type=jnp.float32)
    real = first[:, :, :, 0] - second[:, :, :, 1]
    imag = first[:, :, :, 1] + second[:, :, :, 0]
    zlines = jnp.stack((real, imag), axis=3).astype(jnp.bfloat16)
    zlines = zlines.reshape(2, depth, height_local, 2 * per)
    block = lax.all_to_all(zlines, "col", split_axis=1, concat_axis=3, tiled=True)
    result = jnp.dot(block.reshape(-1, width), back_x, preferred_element_type=jnp.float32)
    result = result.astype(jnp.bfloat16).reshape(block.shape)
    return (result[0], result[1])


def flip(at, d):
    moved = at
    for bit in range(d.bit_length()):
        step = 1 << bit
        if d & step:
            moved = moved + (1 - 2 * ((at // step) % 2)) * step
    return moved


def order(n):
    return list(range(n - 1, 0, -1))


def transform_kernel(
    dims, p_hbm, s_hbm, tab_hbm, gf_hbm, gi_hbm, bx_hbm, fy, by, rates, o0, o1,
    f0, f1, tab, gf, gi, bx, wf, wb,
    tmp, send1, recv1, bsend, brecv, esend, erecv, hsend, hrecv, acc,
    in_sem, tab_sem,
    s1s, s1r, s1l, s2s, s2r, s2l, s3s, s3r, s3l, s4s, s4r, s4l,
):
    cols, rows, chunks, mc, zl, yl, height, depth, width = dims
    nl = KEEP // rows
    per = mc * chunks
    lanes = 2 * yl
    qc = 2 * mc
    blocks = zl // 16
    col_at = lax.axis_index("col")
    row_at = lax.axis_index("row")

    def span(zb):
        return pl.ds(pl.multiple_of(zb * 16, 16), 16)

    def load(field, zb):
        src, dst = ((p_hbm, f0), (s_hbm, f1))[field]
        return pltpu.make_async_copy(src.at[span(zb)], dst.at[span(zb)], in_sem.at[field, zb])

    consts = [
        pltpu.make_async_copy(src, dst, tab_sem.at[i])
        for i, (src, dst) in enumerate(((tab_hbm, tab), (gf_hbm, gf), (gi_hbm, gi), (bx_hbm, bx)))
    ]
    consts[0].start()
    for zb in range(blocks):
        load(0, zb).start()
        load(1, zb).start()
    for c in consts[1:]:
        c.start()

    barrier = pltpu.get_barrier_semaphore()
    for d in range(1, cols):
        pl.semaphore_signal(barrier, inc=1, device_id={"col": flip(col_at, d)}, device_id_type=MESH)
    for d in range(1, rows):
        pl.semaphore_signal(barrier, inc=1, device_id={"row": flip(row_at, d)}, device_id_type=MESH)
    pl.semaphore_wait(barrier, cols + rows - 2)

    def exchange(axis, n, at, src, dst, ss, rs, ls, k):
        own = lambda: pltpu.make_async_copy(src(at), dst(at), ls.at[k])
        pairs = []
        for d in order(n):
            peer = flip(at, d)
            pairs.append(
                pltpu.make_async_remote_copy(
                    src_ref=src(peer),
                    dst_ref=dst(at),
                    send_sem=ss.at[k, d],
                    recv_sem=rs.at[k, d],
                    device_id={axis: peer},
                    device_id_type=MESH,
                )
            )
        return own, pairs

    def ex1(k, zb):
        return exchange(
            "col", cols, col_at,
            lambda p: send1.at[k, pl.ds(p * qc, qc), span(zb), :],
            lambda p: recv1.at[k, :, pl.ds(pl.multiple_of(p * zl + zb * 16, 16), 16), :],
            s1s, s1r, s1l, k * blocks + zb,
        )

    def ex2(k):
        return exchange(
            "row", rows, row_at,
            lambda p: bsend.at[k, :, :, pl.ds(pl.multiple_of(p * nl, 16), nl), :],
            lambda p: brecv.at[k, p],
            s2s, s2r, s2l, k,
        )

    def ex3(k):
        return exchange(
            "row", rows, row_at,
            lambda p: esend.at[k, p],
            lambda p: erecv.at[k, :, :, pl.ds(pl.multiple_of(p * nl, 16), nl), :],
            s3s, s3r, s3l, k,
        )

    def ex4(k, zb):
        return exchange(
            "col", cols, col_at,
            lambda p: hsend.at[k, :, :, pl.ds(pl.multiple_of(p * zl + zb * 16, 16), 16), :],
            lambda p: hrecv.at[k, p, :, :, span(zb), :],
            s4s, s4r, s4l, k * blocks + zb,
        )

    def begin(ex):
        own, pairs = ex
        for c in pairs:
            c.start()
        own().start()

    def arrive(ex):
        own, pairs = ex
        own().wait()
        for c in pairs:
            c.wait_recv()

    def leave(ex):
        for c in ex[1]:
            c.wait_send()

    consts[0].wait()

    def forward(i, carry):
        k, zb = i // blocks, i % blocks

        @pl.when(k == 0)
        def _():
            load(0, zb).wait()
            load(1, zb).wait()

        for zi in range(0, 16, 2):
            z = zb * 16 + zi
            lines = jnp.concatenate((f0[z], f1[z], f0[z + 1], f1[z + 1]), axis=0)
            out = lax.dot_general(
                tab[k], lines, (((1,), (1,)), ((), ())), preferred_element_type=jnp.float32
            )
            tmp[:, zi, :] = out[:, :lanes]
            tmp[:, zi + 1, :] = out[:, lanes:]
        send1[k, :, span(zb), :] = tmp[...].astype(jnp.bfloat16)
        begin(ex1(k, zb))
        return carry

    lax.fori_loop(0, chunks * blocks, forward, 0)
    for c in consts[1:]:
        c.wait()

    wf[...] = jnp.zeros_like(wf)
    lines = fy[...].T
    for s in range(rows):
        for f in range(2):
            wf[s * lanes + f * yl:s * lanes + (f + 1) * yl, f * height:(f + 1) * height] = lines[
                s * yl:(s + 1) * yl
            ]
    lines = by[...].T
    blank = jnp.zeros((height, yl), jnp.bfloat16)
    for r in range(rows):
        part = lines[:, r * yl:(r + 1) * yl]
        wb[:height, r * lanes:(r + 1) * lanes] = jnp.concatenate((part, blank), axis=1)
        wb[height:, r * lanes:(r + 1) * lanes] = jnp.concatenate((blank, part), axis=1)

    def zforward(k):
        def pair(i, carry):
            m = 2 * i
            x = jnp.concatenate(
                [
                    jnp.concatenate((recv1[k, m + a], recv1[k, mc + m + a]), axis=0)
                    for a in range(2)
                ],
                axis=1,
            )
            b = jnp.dot(gf[...], x, preferred_element_type=jnp.float32).astype(jnp.bfloat16)
            for a in range(2):
                for p in range(2):
                    bsend[k, m + a, p] = b[p * KEEP:(p + 1) * KEEP, a * lanes:(a + 1) * lanes]
            return carry

        lax.fori_loop(0, mc // 2, pair, 0)

    def solve(k):
        n = row_at * nl + lax.broadcasted_iota(jnp.int32, (nl, 1), 0)
        n = jnp.where(n < KEEP // 2, n, n + (depth - KEEP))
        n = jnp.where(n < depth // 2, n, n - depth)
        kz_sq = (n.astype(jnp.float32) * (2.0 * math.pi / depth)) ** 2

        def one(m, carry):
            mode = jnp.full((1, 1), col_at * per + k * mc + m, jnp.int32)
            kx_sq = (mode.astype(jnp.float32) * (2.0 * math.pi / width)) ** 2
            total = (kx_sq + kz_sq) + jnp.concatenate((rates[...], rates[...]), axis=1)
            field = lax.broadcasted_iota(jnp.int32, total.shape, 1) // height
            inv = 1.0 / jnp.where(field == 0, -total, 1.0 + diffusion * total)
            line = jnp.concatenate(
                [brecv[k, s, m].reshape(2 * nl, lanes) for s in range(rows)], axis=1
            )
            c = jnp.dot(line, wf[...], preferred_element_type=jnp.float32)
            hat = (c * jnp.concatenate((inv, inv), axis=0)).astype(jnp.bfloat16)
            e = jnp.dot(hat, wb[...], preferred_element_type=jnp.float32).astype(jnp.bfloat16)
            for r in range(rows):
                esend[k, r, m] = e[:, r * lanes:(r + 1) * lanes].reshape(2, nl, lanes)
            return carry

        lax.fori_loop(0, mc, one, 0)

    def zback(k):
        def pair(i, carry):
            m = 2 * i
            x = jnp.concatenate(
                [erecv[k, m + a].reshape(2 * KEEP, lanes) for a in range(2)], axis=1
            )
            h = jnp.dot(gi[...], x, preferred_element_type=jnp.float32).astype(jnp.bfloat16)
            for a in range(2):
                for p in range(2):
                    hsend[k, p, m + a] = h[p * depth:(p + 1) * depth, a * lanes:(a + 1) * lanes]
            return carry

        lax.fori_loop(0, mc // 2, pair, 0)

    def each(k, act):
        def one(zb, carry):
            act(k, zb)
            return carry

        lax.fori_loop(0, blocks, one, 0)

    def middle(k, carry):
        each(k, lambda k, zb: arrive(ex1(k, zb)))
        zforward(k)
        begin(ex2(k))
        arrive(ex2(k))
        solve(k)
        begin(ex3(k))
        arrive(ex3(k))
        zback(k)
        each(k, lambda k, zb: begin(ex4(k, zb)))
        return carry

    lax.fori_loop(0, chunks, middle, 0)

    def result(k, zb):
        arrive(ex4(k, zb))
        tmp[...] = hrecv[k, :, :, :, span(zb), :].reshape(tmp.shape).astype(jnp.float32)
        for zi in range(0, 16, 2):
            z = zb * 16 + zi
            x = jnp.concatenate((tmp[:, zi, :], tmp[:, zi + 1, :]), axis=1).astype(jnp.bfloat16)
            out = lax.dot_general(
                x, bx[k], (((0,), (0,)), ((), ())), preferred_element_type=jnp.float32
            )
            for a in range(2):
                half = out[a * lanes:(a + 1) * lanes]
                if k > 0:
                    half = acc[z + a] + half
                if k < chunks - 1:
                    acc[z + a] = half
                else:
                    o0[z + a] = half[:yl].astype(jnp.bfloat16)
                    o1[z + a] = half[yl:].astype(jnp.bfloat16)

    for k in range(chunks):
        each(k, result)

    def finish(k, carry):
        each(k, lambda k, zb: leave(ex1(k, zb)))
        leave(ex2(k))
        leave(ex3(k))
        each(k, lambda k, zb: leave(ex4(k, zb)))
        return carry

    lax.fori_loop(0, chunks, finish, 0)

def store_kernel(a, b, o0, o1, sem):
    copies = []
    parts = sem.shape[1]
    for f, (src, dst) in enumerate(((a, o0), (b, o1))):
        size = src.shape[0] // parts
        for i in range(parts):
            at = pl.ds(i * size, size)
            copies.append(pltpu.make_async_copy(src.at[at], dst.at[at], sem.at[f, i]))
    for c in copies:
        c.start()
    for c in copies:
        c.wait()


def tables(cols, chunks, mc, depth, width):
    per = mc * chunks
    mode = np.arange(width // 2).reshape(cols, chunks, mc)
    mode = np.stack((mode, mode), axis=2).transpose(1, 0, 2, 3).reshape(-1)
    part = np.broadcast_to(np.arange(2)[None, None, :, None], (chunks, cols, 2, mc)).reshape(-1)
    place = np.arange(width)
    angle = (mode[:, None] * place[None, :] % width).astype(np.float32) * np.float32(
        2.0 * math.pi / width
    )
    factor = np.float32(math.sqrt(2.0 / width))
    wave_x = np.where(part[:, None] == 0, factor * np.cos(angle), -factor * np.sin(angle))
    weight = np.where(mode == 0, 0.5, 1.0).astype(np.float32)[:, None]
    tab = wave_x.astype(jnp.bfloat16).reshape(chunks, -1, width)
    back = (wave_x * weight).astype(jnp.bfloat16).reshape(chunks, -1, width)
    wave = np.arange(KEEP)
    wave = np.where(wave < KEEP // 2, wave, wave + (depth - KEEP))
    angle = (wave[:, None] * np.arange(depth)[None, :] % depth).astype(np.float32) * np.float32(
        2.0 * math.pi / depth
    )
    factor = np.float32(1.0 / math.sqrt(depth))
    c, s = factor * np.cos(angle), factor * np.sin(angle)
    gf = np.block([[c, s], [-s, c]]).astype(jnp.bfloat16)
    gi = np.block([[c.T, -s.T], [s.T, c.T]]).astype(jnp.bfloat16)
    return tab, back, gf, gi


def fused(pressure_rhs, scalar_source, forward_y, back_y, wall_rates):
    rows = lax.axis_size("row")
    cols = lax.axis_size("col")
    zl, yl, width = pressure_rhs.shape
    height = forward_y.shape[0]
    depth = zl * cols
    per = width // (2 * cols)
    chunks = CHUNKS
    mc = per // chunks
    nl = KEEP // rows
    lanes = 2 * yl
    tab, back, gf, gi = tables(cols, chunks, mc, depth, width)
    rates = wall_rates.reshape(1, height)
    dims = (cols, rows, chunks, mc, zl, yl, height, depth, width)
    bf = jnp.bfloat16
    dma = pltpu.SemaphoreType.DMA
    blocks = zl // 16
    sems = [dma((2, blocks)), dma((4,))]
    for n, steps in ((cols, chunks * blocks), (rows, chunks), (rows, chunks), (cols, chunks * blocks)):
        sems += [dma((steps, n)), dma((steps, n)), dma((steps,))]
    field = jax.ShapeDtypeStruct((zl, yl, width), bf)
    anywhere = pl.BlockSpec(memory_space=pl.ANY)
    inside = pl.BlockSpec(memory_space=pltpu.VMEM)
    vmem = [
        (field.shape, bf),
        (field.shape, bf),
        (tab.shape, bf),
        (gf.shape, bf),
        (gi.shape, bf),
        (back.shape, bf),
        ((rows * lanes, 2 * height), bf),
        ((2 * height, rows * lanes), bf),
        ((cols * 2 * mc, 16, lanes), jnp.float32),
        ((chunks, cols * 2 * mc, zl, lanes), bf),
        ((chunks, 2 * mc, depth, lanes), bf),
        ((chunks, mc, 2, KEEP, lanes), bf),
        ((chunks, rows, mc, 2, nl, lanes), bf),
        ((chunks, rows, mc, 2, nl, lanes), bf),
        ((chunks, mc, 2, KEEP, lanes), bf),
        ((chunks, 2, mc, depth, lanes), bf),
        ((chunks, cols, 2, mc, zl, lanes), bf),
        ((zl, lanes, width), jnp.float32),
    ]
    held = pltpu.VMEM(field.shape, bf)
    whole = pl.pallas_call(
        functools.partial(transform_kernel, dims),
        out_shape=[held, held],
        in_specs=[anywhere] * 6 + [inside] * 3,
        out_specs=[inside] * 2,
        scratch_shapes=[pltpu.VMEM(*v) for v in vmem] + sems,
        compiler_params=pltpu.CompilerParams(
            collective_id=0, has_side_effects=True, vmem_limit_bytes=56 << 20
        ),
    )(pressure_rhs, scalar_source, tab, gf, gi, back, forward_y, back_y, rates)
    return tuple(
        pl.pallas_call(
            store_kernel,
            out_shape=[field, field],
            in_specs=[inside] * 2,
            out_specs=[anywhere] * 2,
            scratch_shapes=[dma((2, blocks))],
            compiler_params=pltpu.CompilerParams(vmem_limit_bytes=1 << 20),
        )(*whole)
    )


def fits(rows, cols, pressure_rhs, forward_y):
    depth, height, width = pressure_rhs.shape
    power = rows & (rows - 1) == 0 and cols & (cols - 1) == 0
    if depth % cols or height % rows or width % (2 * cols * CHUNKS) or KEEP % rows:
        return False
    return (
        power
        and (2 * height // rows) % 128 == 0
        and (depth // cols) % 16 == 0
        and (KEEP // rows) % 16 == 0
        and (width // (2 * cols * CHUNKS)) % 2 == 0
    )


def solution(mesh):
    placed = (P("col", "row", None), P("col", "row", None), P(), P(), P())
    rows, cols = mesh.shape["row"], mesh.shape["col"]

    def run(pressure_rhs, scalar_source, forward_y, back_y, wall_rates):
        body = fused if fits(rows, cols, pressure_rhs, forward_y) else shards
        return jax.shard_map(
            body,
            mesh=mesh,
            in_specs=placed,
            out_specs=(P("col", "row", None), P("col", "row", None)),
            check_vma=False,
        )(pressure_rhs, scalar_source, forward_y, back_y, wall_rates)

    return run
```
